16 devices in a mesh: dp: 4 (over z, y), ep: 4 (over x, core).
Axes of the slice: x: 2, y: 2, z: 2, core: 2. Of those that a mesh axis runs over, the one named last changes fastest.
Arguments:
- dispatched: bfloat16 [16, 8, 1024, 2048], P('dp', 'ep'), parts along dimension 0
- w_gate: bfloat16 [8, 2048, 5632], P('ep')
- w_up: bfloat16 [8, 2048, 5632], P('ep')
- w_down: bfloat16 [8, 5632, 2048], P('ep')
- fill_count: int32 [16, 8], P('dp', 'ep'), parts along dimension 0
- slot_index: int32 [32768, 2], P(('dp', 'ep')), parts along dimension 0
- expert_id: int32 [32768, 2], P(('dp', 'ep')), parts along dimension 0
- gate_weight: float32 [32768, 2], P(('dp', 'ep')), parts along dimension 0
Outputs:
- output: bfloat16 [32768, 2048], P(('dp', 'ep')), parts along dimension 0
There are 4 independent parts. The reference program is written for one: setup_inputs(seed, part) draws one part's arguments, and reference() takes and returns one part's arrays. A program takes and returns all parts, laid end to end along the dimension named above; an argument that names none is the same for every part.
All inputs are finite; a program needn't handle non-finite values.
Results may differ from the reference program's by a relative error of at most 0.00134.
Values are sent between devices in bfloat16 or wider.
A program may use at most 1 GiB of HBM per device.

```python
import jax
import jax.numpy as jnp
from jax import lax

HIDDEN = 2048
FFN_DIM = 5632
EXPERTS = 8
TOP_K = 2
TOKENS_DEV = 2048
GROUP_SIZE = 4
CAPACITY = (2 * TOKENS_DEV * TOP_K) // EXPERTS


def draw_routing(route_key):
    key_perm, key_noise, key_shift = jax.random.split(route_key, 3)
    popularity = jax.random.permutation(key_perm, EXPERTS)
    base_score = 4000 // (popularity + 1)
    noise_term = jax.random.randint(key_noise, (GROUP_SIZE, TOKENS_DEV, EXPERTS), 0, 1000)
    cover_shift = jax.random.randint(key_shift, (GROUP_SIZE, 1), 0, EXPERTS)
    expert_ids = jnp.arange(EXPERTS, dtype=jnp.int32)
    cover_id = (jnp.arange(TOKENS_DEV, dtype=jnp.int32)[None, :] + cover_shift) % EXPERTS
    cover_bonus = jnp.where(expert_ids[None, None, :] == cover_id[:, :, None], 100000, 0)
    route_score = (base_score[None, None, :] + noise_term + cover_bonus) * EXPERTS + expert_ids
    chosen = lax.top_k(route_score, TOP_K)[1]
    onehot = (chosen.reshape(GROUP_SIZE, TOKENS_DEV * TOP_K, 1) == expert_ids).astype(jnp.int32)
    earlier = jnp.cumsum(onehot, axis=1) - onehot
    arrival = jnp.sum(earlier * onehot, axis=2)
    slot_index = jnp.where(arrival < CAPACITY, arrival, -1)
    filled_count = jnp.minimum(jnp.sum(onehot, axis=1), CAPACITY)
    expert_id = chosen.reshape(GROUP_SIZE * TOKENS_DEV, TOP_K).astype(jnp.int32)
    slot_index = slot_index.reshape(GROUP_SIZE * TOKENS_DEV, TOP_K).astype(jnp.int32)
    return expert_id, slot_index, filled_count.astype(jnp.int32)


def setup_inputs(seed: int = 0, part: int = 0) -> dict:
    shared_key, part_root = jax.random.split(jax.random.key(seed))
    key_gate_w, key_up_w, key_down_w = jax.random.split(shared_key, 3)
    part_key = jax.random.fold_in(part_root, part)
    key_route, key_rows, key_mix = jax.random.split(part_key, 3)
    expert_id, slot_index, filled_count = draw_routing(key_route)
    dispatched = jax.random.normal(key_rows, (GROUP_SIZE, EXPERTS, CAPACITY, HIDDEN), jnp.float32)
    w_gate = jax.random.normal(key_gate_w, (EXPERTS, HIDDEN, FFN_DIM), jnp.float32) * HIDDEN ** -0.5
    w_up = jax.random.normal(key_up_w, (EXPERTS, HIDDEN, FFN_DIM), jnp.float32) * HIDDEN ** -0.5
    w_down = jax.random.normal(key_down_w, (EXPERTS, FFN_DIM, HIDDEN), jnp.float32) * FFN_DIM ** -0.5
    logits = jax.random.normal(key_mix, (GROUP_SIZE * TOKENS_DEV, TOP_K), jnp.float32) * 1.5
    return {
        "dispatched": dispatched.astype(jnp.bfloat16),
        "w_gate": w_gate.astype(jnp.bfloat16),
        "w_up": w_up.astype(jnp.bfloat16),
        "w_down": w_down.astype(jnp.bfloat16),
        "fill_count": filled_count,
        "slot_index": slot_index,
        "expert_id": expert_id,
        "gate_weight": jax.nn.softmax(logits, axis=-1),
    }


def reference(dispatched, w_gate, w_up, w_down, fill_count, slot_index, expert_id, gate_weight):
    group_size = dispatched.shape[0]
    capacity = dispatched.shape[2]
    tokens_dev = slot_index.shape[0] // group_size

    def expert_ffn(operands):
        row_block, gate_w, up_w, down_w, filled = operands
        rows_f32 = row_block.astype(jnp.float32)
        pre_gate = jnp.einsum("scd,df->scf", rows_f32, gate_w.astype(jnp.float32))
        pre_up = jnp.einsum("scd,df->scf", rows_f32, up_w.astype(jnp.float32))
        hidden = (jax.nn.silu(pre_gate) * pre_up).astype(jnp.bfloat16)
        result = jnp.einsum("scf,fd->scd", hidden.astype(jnp.float32), down_w.astype(jnp.float32)).astype(jnp.bfloat16)
        live_mask = jnp.arange(capacity)[None, :] < filled[:, None]
        return jnp.where(live_mask[:, :, None], result, jnp.zeros_like(result))

    expert_out = lax.map(expert_ffn, (jnp.swapaxes(dispatched, 0, 1), w_gate, w_up, w_down, jnp.swapaxes(fill_count, 0, 1)))
    flat_rows = expert_out.reshape(-1, expert_out.shape[-1])
    source = (jnp.arange(slot_index.shape[0]) // tokens_dev)[:, None]
    row_index = (expert_id * group_size + source) * capacity + jnp.maximum(slot_index, 0)
    weight = jnp.where(slot_index >= 0, gate_weight, 0.0)
    combined = jnp.zeros((slot_index.shape[0], flat_rows.shape[1]), jnp.float32)
    for choice in range(slot_index.shape[1]):
        picked = jnp.take(flat_rows, row_index[:, choice], axis=0).astype(jnp.float32)
        combined = combined + weight[:, choice, None] * picked
    return combined.astype(jnp.bfloat16)
```

```python
import functools

import jax
import jax.numpy as jnp
from jax import lax
from jax.experimental import pallas as pl
from jax.experimental.pallas import tpu as pltpu
from jax.sharding import PartitionSpec as P


BIG, SMALL = 512, 256
CHUNK = 256
TOKENS = 512
VMEM_LIMIT = 58 * 1024 * 1024


def ffn_kernel(table, x_ref, gate_ref, up_ref, down_ref, y_ref, total):
    p, f = pl.program_id(0), pl.program_id(1)
    rows_filled = table[2, p]

    def tile(start, size):
        rows = pl.ds(pl.multiple_of(start, SMALL), size)
        x = x_ref[0, 0, rows, :]
        a = jnp.dot(x, gate_ref[0], preferred_element_type=jnp.float32)
        b = jnp.dot(x, up_ref[0], preferred_element_type=jnp.float32)
        h = (jax.nn.silu(a) * b).astype(jnp.bfloat16)
        y = jnp.dot(h, down_ref[0], preferred_element_type=jnp.float32)
        total[rows, :] = jnp.where(f == 0, 0.0, total[rows, :]) + y

    units = (rows_filled + SMALL - 1) >> 8
    pairs = units >> 1

    def pair(i, carry):
        tile(i * BIG, BIG)
        return carry

    lax.fori_loop(0, pairs, pair, 0)

    @pl.when((units & 1) == 1)
    def _():
        tile(pairs * BIG, SMALL)

    @pl.when(f == pl.num_programs(1) - 1)
    def _():
        def store(i, carry):
            rows = pl.ds(pl.multiple_of(i * SMALL, SMALL), SMALL)
            slot = i * SMALL + lax.broadcasted_iota(jnp.int32, (SMALL, 1), 0)
            y_ref[0, 0, rows, :] = jnp.where(slot < rows_filled, total[rows, :], 0.0).astype(jnp.bfloat16)
            return carry

        lax.fori_loop(0, units, store, 0)


def ffn(table, out_sources, x, w_gate, w_up, w_down, width=512):
    _, experts, capacity, hidden = x.shape
    width_all = w_gate.shape[2]
    last = width_all // width - 1

    def slice_of(p, f, t):
        return jnp.where(t[4, p] == 1, f, last)

    weight = pl.BlockSpec((1, hidden, width), lambda p, f, t: (t[1, p], 0, slice_of(p, f, t)))
    block = (1, 1, capacity, hidden)
    return pl.pallas_call(
        ffn_kernel,
        out_shape=jax.ShapeDtypeStruct((out_sources, experts, capacity, hidden), jnp.bfloat16),
        grid_spec=pltpu.PrefetchScalarGridSpec(
            num_scalar_prefetch=1,
            grid=(table.shape[1], last + 1),
            in_specs=[
                pl.BlockSpec(block, lambda p, f, t: (t[0, p], t[1, p], 0, 0)),
                weight,
                weight,
                pl.BlockSpec((1, width, hidden), lambda p, f, t: (t[1, p], slice_of(p, f, t), 0)),
            ],
            out_specs=pl.BlockSpec(block, lambda p, f, t: (t[3, p], t[1, p], 0, 0)),
            scratch_shapes=[pltpu.VMEM((capacity, hidden), jnp.float32)],
        ),
        compiler_params=pltpu.CompilerParams(
            dimension_semantics=("arbitrary", "arbitrary"), vmem_limit_bytes=VMEM_LIMIT
        ),
        cost_estimate=pl.CostEstimate(
            flops=6 * 1536 * out_sources * hidden * width_all,
            bytes_accessed=12 * out_sources * hidden * width_all,
            transcendentals=0,
        ),
    )(table, x, w_gate, w_up, w_down)


def combine_kernel(final, info, meta_ref, own_ref, part_ref, *refs):
    if final:
        helped_ref, z0_ref, z1_ref, out_ref, total = refs
    else:
        out_ref, total = refs
    q, t = pl.program_id(0), pl.program_id(1)
    tokens = pl.ds(pl.multiple_of(t * TOKENS, TOKENS), TOKENS)
    lane = lax.broadcasted_iota(jnp.int32, (TOKENS, meta_ref.shape[1]), 1)
    meta = meta_ref[...]
    slot = jnp.sum(jnp.where(lane == q, meta, 0.0), axis=1, keepdims=True)
    scale = jnp.sum(jnp.where(lane == q + 4, meta, 0.0), axis=1, keepdims=True)

    @pl.when((q == 0) & (info[7] == 1))
    def _():
        total[tokens, :] = jnp.zeros((TOKENS, total.shape[1]), jnp.float32)

    def add_from(ref):
        def add(k, carry):
            rows = pl.ds(pl.multiple_of(k * CHUNK, CHUNK), CHUNK)
            ids = (k * CHUNK + lax.broadcasted_iota(jnp.int32, (TOKENS, CHUNK), 1)).astype(jnp.float32)
            select = jnp.where(slot == ids, 1.0, 0.0).astype(jnp.bfloat16)
            picked = jnp.dot(select, ref[0, 0, rows, :], preferred_element_type=jnp.float32)
            total[tokens, :] += scale * picked
            return carry

        lax.fori_loop(0, (info[q] + CHUNK - 1) >> 8, add, 0)

    @pl.when(q < 2)
    def _():
        add_from(own_ref)

    if final:
        @pl.when((q >= 2) & (info[6] == 0))
        def _():
            add_from(part_ref)

        @pl.when((q >= 2) & (info[6] == 1))
        def _():
            add_from(helped_ref)
    else:
        @pl.when(q >= 2)
        def _():
            add_from(part_ref)

    @pl.when((q == 3) & (info[7] == 1))
    def _():
        if final:
            back = jnp.sum(jnp.where(lane == 8, meta, 0.0), axis=1, keepdims=True)

            def finish(z_ref):
                z = jnp.where(back > 0.0, z_ref[...].astype(jnp.float32), 0.0)
                out_ref[...] = (total[tokens, :] + back * z).astype(jnp.bfloat16)

            @pl.when(info[5] == 0)
            def _():
                finish(z0_ref)

            @pl.when(info[5] == 1)
            def _():
                finish(z1_ref)
        else:
            out_ref[...] = total[tokens, :].astype(jnp.bfloat16)


def combine(final, info, meta, own, part, *more):
    capacity, hidden = own.shape[2:]
    count, lanes = meta.shape
    block = (1, 1, capacity, hidden)
    in_specs = [
        pl.BlockSpec((TOKENS, lanes), lambda q, t, i: (t * i[7], 0)),
        pl.BlockSpec(block, lambda q, t, i: (i[4], jnp.minimum(q, 1) * i[7], 0, 0)),
        pl.BlockSpec(block, lambda q, t, i: (0, jnp.maximum(q - 2, 0) * i[7], 0, 0)),
    ]
    if final:
        in_specs += [
            pl.BlockSpec(block, lambda q, t, i: (0, jnp.maximum(q - 2, 0) * i[6], 0, 0)),
            pl.BlockSpec((TOKENS, hidden), lambda q, t, i: (jnp.where((q == 3) & (i[5] == 0), t, 0), 0)),
            pl.BlockSpec((TOKENS, hidden), lambda q, t, i: (jnp.where((q == 3) & (i[5] == 1), t, 0), 0)),
        ]
    return pl.pallas_call(
        functools.partial(combine_kernel, final),
        out_shape=jax.ShapeDtypeStruct((count, hidden), jnp.bfloat16),
        grid_spec=pltpu.PrefetchScalarGridSpec(
            num_scalar_prefetch=1,
            grid=(4, count // TOKENS),
            in_specs=in_specs,
            out_specs=pl.BlockSpec((TOKENS, hidden), lambda q, t, i: (jnp.where(q == 3, t * i[7], 0), 0)),
            scratch_shapes=[pltpu.VMEM((count, hidden), jnp.float32)],
        ),
        compiler_params=pltpu.CompilerParams(
            dimension_semantics=("arbitrary", "arbitrary"), vmem_limit_bytes=VMEM_LIMIT
        ),
        cost_estimate=pl.CostEstimate(
            flops=2 * 2048 * count * hidden, bytes_accessed=32 * count * hidden, transcendentals=0
        ),
    )(info, meta, own, part, *more)


def routing_meta(experts, slot_index, expert_id, gate_weight, on_chip, raw_single):
    here = (expert_id[:, :, None] == experts) & (slot_index >= 0)[:, :, None]
    slot = jnp.sum(jnp.where(here, slot_index[:, :, None] + 1, 0), axis=1) - 1
    factor = jnp.sum(jnp.where(here, gate_weight[:, :, None], 0.0), axis=1)
    if raw_single:
        factor = jnp.where(on_chip[:, None] == 2, factor, 1.0)
    return jnp.concatenate([slot.astype(jnp.float32), factor], axis=1)


def solution(mesh):
    def local_step(dispatched, w_gate, w_up, w_down, fill_count, slot_index, expert_id, gate_weight):
        me = lax.axis_index("ep")
        core, chip = me & 1, me >> 1
        partner, across = me ^ 1, me ^ 2
        first = 2 * (1 - chip)
        swap_core = [(0, 1), (1, 0), (2, 3), (3, 2)]
        swap_chip = [(0, 2), (2, 0), (1, 3), (3, 1)]

        def permute(value, pairs):
            return lax.ppermute(value, "ep", pairs)

        fill_there = permute(fill_count, swap_core)
        load_here, load_there = jnp.sum(fill_count), jnp.sum(fill_there)
        i_help = load_here + jnp.sum(fill_there[me]) < load_there
        get_help = load_there + jnp.sum(fill_count[partner]) < load_here

        valid = slot_index >= 0
        on_far = jnp.sum((valid & ((expert_id >> 2) != chip)).astype(jnp.int32), axis=1)
        pair_order = jnp.array([0, 1, 2, 3], jnp.int32)

        def chip_experts(owner):
            return jnp.where(pair_order < 2, 2 * owner + pair_order, 2 * (owner ^ 1) + pair_order - 2)

        far_meta = routing_meta(chip_experts(across), slot_index, expert_id, gate_weight, on_far, True)
        near_meta = routing_meta(chip_experts(me), slot_index, expert_id, gate_weight, on_far, False)
        far_weight = jnp.sum(jnp.where(valid & ((expert_id >> 2) != chip), gate_weight, 0.0), axis=1)
        back = jnp.where(on_far == 2, 1.0, jnp.where(on_far == 1, far_weight, 0.0))
        near_meta = jnp.concatenate([near_meta, back[:, None]], axis=1)
        served_meta = permute(far_meta, swap_chip)

        def table(sources, targets, experts_fills, active):
            columns = []
            for source, target, fills, on in zip(sources, targets, experts_fills, active):
                for e in range(2):
                    columns.append(jnp.stack([source, jnp.int32(e), fills[e] * on, target, on]))
            return jnp.stack(columns, axis=1).astype(jnp.int32)

        def info(source, slot_of_own, helped, active):
            fills = jnp.concatenate([fill_count[source], fill_there[source]]) * active
            return jnp.concatenate([fills, jnp.stack([slot_of_own, core, helped, active])]).astype(jnp.int32)

        zero, one = jnp.int32(0), jnp.int32(1)
        gate_there = permute(w_gate, swap_core)
        rows_there = permute(lax.dynamic_slice_in_dim(dispatched, partner, 1, 0), swap_core)

        first_table = table([first], [zero], [fill_count[first]], [one])
        second_table = table([first + 1], [zero], [fill_count[first + 1]], [one])
        y_first = ffn(first_table, 1, dispatched, w_gate, w_up, w_down)
        y_first_part = permute(y_first, [(1, 0), (3, 2)])
        up_sent, down_sent, y_first = lax.optimization_barrier((w_up, w_down, y_first))
        up_there, down_there = permute(up_sent, swap_core), permute(down_sent, swap_core)
        served0 = combine(False, info(first, zero, zero, 1 - core), served_meta, y_first, y_first_part)
        z0 = permute(served0, [(0, 2), (2, 0)])
        second_table, served0 = lax.optimization_barrier((second_table, served0))
        y_second = ffn(second_table, 1, dispatched, w_gate, w_up, w_down)
        y_second_part = permute(y_second, [(0, 1), (2, 3)])
        served1 = combine(False, info(first + 1, zero, zero, core), served_meta, y_second, y_second_part)
        z1 = permute(served1, [(1, 3), (3, 1)])

        serve_partner = 1 - get_help.astype(jnp.int32)
        local_table = jnp.where(
            (serve_partner == 0) & (jnp.arange(4) >= 2),
            jnp.stack([me, one, zero, zero, zero])[:, None],
            table([me, partner], [zero, one], [fill_count[me], fill_count[partner]], [one, one]),
        ).astype(jnp.int32)
        local_table, served1 = lax.optimization_barrier((local_table, served1))
        y_local = ffn(local_table, 2, dispatched, w_gate, w_up, w_down)
        y_part = permute(y_local[1:2], swap_core)
        helps = i_help.astype(jnp.int32)
        help_table = table([zero], [zero], [fill_there[me]], [helps])
        help_table = jnp.where((helps == 0) & (jnp.arange(5) == 1)[:, None], 0, help_table)
        help_table, y_local = lax.optimization_barrier((help_table, y_local))
        y_help = ffn(help_table, 1, rows_there, gate_there, up_there, down_there)
        return combine(True, info(me, zero, helps, one), near_meta, y_local, y_part, y_help, z0, z1)

    token_spec = P(("dp", "ep"))
    in_specs = (P("dp", "ep"), P("ep"), P("ep"), P("ep"), P("dp", "ep"), token_spec, token_spec, token_spec)

    return jax.shard_map(local_step, mesh=mesh, in_specs=in_specs, out_specs=token_spec, check_vma=False)
```

```python
import functools

import jax
import jax.numpy as jnp
from jax import lax
from jax.experimental import pallas as pl
from jax.experimental.pallas import tpu as pltpu
from jax.sharding import PartitionSpec as P


BIG, SMALL = 512, 256
CHUNK = 256
TOKENS = 512
VMEM_LIMIT = 58 * 1024 * 1024


def ffn_kernel(carried, split, table, fill, x_ref, gate_ref, up_ref, down_ref, *refs):
    p, f = pl.program_id(0), pl.program_id(1)
    refs = refs[1:] if carried else refs
    outs, total = refs[:-1], refs[-1]
    rows_filled = fill[table[0, p], table[1, p]] * table[3, p]

    def tile(start, size):
        rows = pl.ds(pl.multiple_of(start, SMALL), size)
        x = x_ref[0, 0, rows, :]
        a = jnp.dot(x, gate_ref[0], preferred_element_type=jnp.float32)
        b = jnp.dot(x, up_ref[0], preferred_element_type=jnp.float32)
        h = (jax.nn.silu(a) * b).astype(jnp.bfloat16)
        y = jnp.dot(h, down_ref[0], preferred_element_type=jnp.float32)
        total[rows, :] = jnp.where(f == 0, 0.0, total[rows, :]) + y

    units = (rows_filled + SMALL - 1) >> 8
    pairs = units >> 1

    def pair(i, carry):
        tile(i * BIG, BIG)
        return carry

    lax.fori_loop(0, pairs, pair, 0)

    @pl.when((units & 1) == 1)
    def _():
        tile(pairs * BIG, SMALL)

    def write(y_ref):
        def store(i, carry):
            rows = pl.ds(pl.multiple_of(i * SMALL, SMALL), SMALL)
            slot = i * SMALL + lax.broadcasted_iota(jnp.int32, (SMALL, 1), 0)
            y_ref[0, 0, rows, :] = jnp.where(slot < rows_filled, total[rows, :], 0.0).astype(jnp.bfloat16)
            return carry

        lax.fori_loop(0, units, store, 0)

    last = f == pl.num_programs(1) - 1
    if len(outs) == 1:
        @pl.when(last)
        def _():
            write(outs[0])
    else:
        @pl.when(last & (p < split))
        def _():
            write(outs[0])

        @pl.when(last & (p >= split))
        def _():
            write(outs[1])


def ffn(table, fill, results, x, w_gate, w_up, w_down, carried=None, width=512):
    _, experts, capacity, hidden = x.shape
    width_all = w_gate.shape[2]
    last = width_all // width - 1

    def slice_of(p, f, t):
        return jnp.where(t[3, p] == 1, f, last)

    weight = pl.BlockSpec((1, hidden, width), lambda p, f, t, n: (t[1, p], 0, slice_of(p, f, t)))
    block = (1, 1, capacity, hidden)
    if len(results) == 1:
        out_specs = [pl.BlockSpec(block, lambda p, f, t, n: (t[2, p], t[1, p], 0, 0))]
    else:
        out_specs = [
            pl.BlockSpec(block, lambda p, f, t, n: (0, jnp.minimum(p, 1), 0, 0)),
            pl.BlockSpec(block, lambda p, f, t, n: (t[2, p], t[1, jnp.maximum(p, 2)], 0, 0)),
        ]
    in_specs = [
        pl.BlockSpec(block, lambda p, f, t, n: (t[0, p], t[1, p], 0, 0)),
        weight,
        weight,
        pl.BlockSpec((1, width, hidden), lambda p, f, t, n: (t[1, p], slice_of(p, f, t), 0)),
    ]
    operands = [table, fill, x, w_gate, w_up, w_down]
    if carried is not None:
        in_specs.append(pl.BlockSpec(memory_space=pl.ANY))
        operands.append(carried)
    return pl.pallas_call(
        functools.partial(ffn_kernel, carried is not None, 2),
        out_shape=[jax.ShapeDtypeStruct((n, experts, capacity, hidden), jnp.bfloat16) for n in results],
        grid_spec=pltpu.PrefetchScalarGridSpec(
            num_scalar_prefetch=2,
            grid=(table.shape[1], last + 1),
            in_specs=in_specs,
            out_specs=out_specs,
            scratch_shapes=[pltpu.VMEM((capacity, hidden), jnp.float32)],
        ),
        input_output_aliases={6: 0} if carried is not None else {},
        compiler_params=pltpu.CompilerParams(
            dimension_semantics=("arbitrary", "arbitrary"), vmem_limit_bytes=VMEM_LIMIT
        ),
        cost_estimate=pl.CostEstimate(
            flops=6 * 1536 * hidden * width_all, bytes_accessed=12 * hidden * width_all, transcendentals=0
        ),
    )(*operands)


def combine_kernel(final, info, meta_ref, own_ref, part_ref, *refs):
    if final:
        helped_ref, z0_ref, z1_ref, out_ref, total = refs
    else:
        out_ref, total = refs
    q, t = pl.program_id(0), pl.program_id(1)
    tokens = pl.ds(pl.multiple_of(t * TOKENS, TOKENS), TOKENS)
    lane = lax.broadcasted_iota(jnp.int32, (TOKENS, meta_ref.shape[1]), 1)
    meta = meta_ref[...]
    slot = jnp.sum(jnp.where(lane == q, meta, 0.0), axis=1, keepdims=True)
    scale = jnp.sum(jnp.where(lane == q + 4, meta, 0.0), axis=1, keepdims=True)

    @pl.when((q == 0) & (info[7] == 1))
    def _():
        total[tokens, :] = jnp.zeros((TOKENS, total.shape[1]), jnp.float32)

    def add_from(ref):
        def add(k, carry):
            rows = pl.ds(pl.multiple_of(k * CHUNK, CHUNK), CHUNK)
            ids = (k * CHUNK + lax.broadcasted_iota(jnp.int32, (TOKENS, CHUNK), 1)).astype(jnp.float32)
            select = jnp.where(slot == ids, 1.0, 0.0).astype(jnp.bfloat16)
            picked = jnp.dot(select, ref[0, 0, rows, :], preferred_element_type=jnp.float32)
            total[tokens, :] += scale * picked
            return carry

        lax.fori_loop(0, (info[q] + CHUNK - 1) >> 8, add, 0)

    @pl.when(q < 2)
    def _():
        add_from(own_ref)

    if final:
        @pl.when((q >= 2) & (info[6] == 0))
        def _():
            add_from(part_ref)

        @pl.when((q >= 2) & (info[6] == 1))
        def _():
            add_from(helped_ref)
    else:
        @pl.when(q >= 2)
        def _():
            add_from(part_ref)

    @pl.when((q == 3) & (info[7] == 1))
    def _():
        if final:
            back = jnp.sum(jnp.where(lane == 8, meta, 0.0), axis=1, keepdims=True)

            def finish(z_ref):
                z = jnp.where(back > 0.0, z_ref[...].astype(jnp.float32), 0.0)
                out_ref[...] = (total[tokens, :] + back * z).astype(jnp.bfloat16)

            @pl.when(info[5] == 0)
            def _():
                finish(z0_ref)

            @pl.when(info[5] == 1)
            def _():
                finish(z1_ref)
        else:
            out_ref[...] = total[tokens, :].astype(jnp.bfloat16)


def combine(final, info, meta, own, part, *more):
    capacity, hidden = own.shape[2:]
    count, lanes = meta.shape
    block = (1, 1, capacity, hidden)
    in_specs = [
        pl.BlockSpec((TOKENS, lanes), lambda q, t, i: (t * i[7], 0)),
        pl.BlockSpec(block, lambda q, t, i: (i[4], jnp.minimum(q, 1) * i[7], 0, 0)),
        pl.BlockSpec(block, lambda q, t, i: (0, jnp.maximum(q - 2, 0) * i[7], 0, 0)),
    ]
    if final:
        in_specs += [
            pl.BlockSpec(block, lambda q, t, i: (0, jnp.maximum(q - 2, 0) * i[6], 0, 0)),
            pl.BlockSpec((TOKENS, hidden), lambda q, t, i: (jnp.where((q == 3) & (i[5] == 0), t, 0), 0)),
            pl.BlockSpec((TOKENS, hidden), lambda q, t, i: (jnp.where((q == 3) & (i[5] == 1), t, 0), 0)),
        ]
    return pl.pallas_call(
        functools.partial(combine_kernel, final),
        out_shape=jax.ShapeDtypeStruct((count, hidden), jnp.bfloat16),
        grid_spec=pltpu.PrefetchScalarGridSpec(
            num_scalar_prefetch=1,
            grid=(4, count // TOKENS),
            in_specs=in_specs,
            out_specs=pl.BlockSpec((TOKENS, hidden), lambda q, t, i: (jnp.where(q == 3, t * i[7], 0), 0)),
            scratch_shapes=[pltpu.VMEM((count, hidden), jnp.float32)],
        ),
        compiler_params=pltpu.CompilerParams(
            dimension_semantics=("arbitrary", "arbitrary"), vmem_limit_bytes=VMEM_LIMIT
        ),
        cost_estimate=pl.CostEstimate(
            flops=2 * 2048 * count * hidden, bytes_accessed=32 * count * hidden, transcendentals=0
        ),
    )(info, meta, own, part, *more)


def routing_meta(experts, slot_index, expert_id, gate_weight, on_chip, raw_single):
    here = (expert_id[:, :, None] == experts) & (slot_index >= 0)[:, :, None]
    slot = jnp.sum(jnp.where(here, slot_index[:, :, None] + 1, 0), axis=1) - 1
    factor = jnp.sum(jnp.where(here, gate_weight[:, :, None], 0.0), axis=1)
    if raw_single:
        factor = jnp.where(on_chip[:, None] == 2, factor, 1.0)
    return jnp.concatenate([slot.astype(jnp.float32), factor], axis=1)


def solution(mesh):
    def local_step(dispatched, w_gate, w_up, w_down, fill_count, slot_index, expert_id, gate_weight):
        me = lax.axis_index("ep")
        core, chip = me & 1, me >> 1
        partner, across = me ^ 1, me ^ 2
        first = 2 * (1 - chip)
        swap_core = [(0, 1), (1, 0), (2, 3), (3, 2)]
        swap_chip = [(0, 2), (2, 0), (1, 3), (3, 1)]

        def permute(value, pairs):
            return lax.ppermute(value, "ep", pairs)

        fill_there = permute(fill_count, swap_core)
        load_here, load_there = jnp.sum(fill_count), jnp.sum(fill_there)
        i_help = load_here + jnp.sum(fill_there[me]) < load_there
        get_help = load_there + jnp.sum(fill_count[partner]) < load_here

        valid = slot_index >= 0
        on_far = jnp.sum((valid & ((expert_id >> 2) != chip)).astype(jnp.int32), axis=1)
        pair_order = jnp.array([0, 1, 2, 3], jnp.int32)

        def chip_experts(owner):
            return jnp.where(pair_order < 2, 2 * owner + pair_order, 2 * (owner ^ 1) + pair_order - 2)

        far_meta = routing_meta(chip_experts(across), slot_index, expert_id, gate_weight, on_far, True)
        near_meta = routing_meta(chip_experts(me), slot_index, expert_id, gate_weight, on_far, False)
        far_weight = jnp.sum(jnp.where(valid & ((expert_id >> 2) != chip), gate_weight, 0.0), axis=1)
        back = jnp.where(on_far == 2, 1.0, jnp.where(on_far == 1, far_weight, 0.0))
        near_meta = jnp.concatenate([near_meta, back[:, None]], axis=1)
        served_meta = permute(far_meta, swap_chip)
        rows_for_partner = lax.dynamic_slice_in_dim(dispatched, partner, 1, 0)
        fill_there_own = lax.dynamic_slice_in_dim(fill_there, me, 1, 0)

        def table(sources, places, active):
            passes = 2 * len(sources)
            row = lax.broadcasted_iota(jnp.int32, (4, passes), 0)
            column = lax.broadcasted_iota(jnp.int32, (4, passes), 1)

            def spread(values):
                return values[0] if len(values) == 1 else jnp.where(column < 2, values[0], values[1])

            return jnp.where(
                row == 0,
                spread(sources),
                jnp.where(row == 1, jnp.where(spread(active) == 1, column & 1, 1), jnp.where(row == 2, spread(places), spread(active))),
            ).astype(jnp.int32)

        def info(source, helped):
            fills = jnp.concatenate([fill_count[source], fill_there[source]])
            return jnp.concatenate([fills, jnp.stack([zero, core, helped, one])]).astype(jnp.int32)

        def serve_info(source, active):
            fills = jnp.concatenate([fill_count[source], fill_there[source]]) * active
            return jnp.concatenate([fills, jnp.stack([zero, core, zero, active])]).astype(jnp.int32)

        zero, one = jnp.int32(0), jnp.int32(1)
        helps = i_help.astype(jnp.int32)
        deferred = get_help.astype(jnp.int32)
        early = 1 - deferred
        gate_there = permute(w_gate, swap_core)

        y_first, y_own = ffn(
            table([first, jnp.where(early == 1, me, first)], [zero, zero], [one, early]),
            fill_count,
            (1, 2),
            dispatched,
            w_gate,
            w_up,
            w_down,
        )
        y_first_part = permute(y_first, [(1, 0), (3, 2)])
        up_sent, down_sent, rows_sent, y_first = lax.optimization_barrier((w_up, w_down, rows_for_partner, y_first))
        up_there = permute(up_sent, swap_core)
        down_there = permute(down_sent, swap_core)
        rows_there = permute(rows_sent, swap_core)
        served0 = combine(False, serve_info(first, 1 - core), served_meta, y_first, y_first_part)
        z0 = permute(served0, [(0, 2), (2, 0)])
        second_table = table(
            [first + 1, jnp.where(early == 1, partner, first + 1)], [zero, zero], [one, early]
        )
        second_table, served0 = lax.optimization_barrier((second_table, served0))
        y_second, y_for_partner = ffn(second_table, fill_count, (1, 1), dispatched, w_gate, w_up, w_down)
        y_second_part = permute(y_second, [(0, 1), (2, 3)])
        served1 = combine(False, serve_info(first + 1, core), served_meta, y_second, y_second_part)
        z1 = permute(served1, [(1, 3), (3, 1)])
        y_part = permute(y_for_partner, swap_core)

        local_table = table([me], [early], [deferred])
        local_table, served1 = lax.optimization_barrier((local_table, served1))
        y_own = ffn(local_table, fill_count, (2,), dispatched, w_gate, w_up, w_down, carried=y_own)[0]
        help_table = table([zero], [zero], [helps])
        help_table, y_own = lax.optimization_barrier((help_table, y_own))
        y_help = ffn(help_table, fill_there_own, (1,), rows_there, gate_there, up_there, down_there)[0]
        return combine(True, info(me, helps), near_meta, y_own, y_part, y_help, z0, z1)

    token_spec = P(("dp", "ep"))
    in_specs = (P("dp", "ep"), P("ep"), P("ep"), P("ep"), P("dp", "ep"), token_spec, token_spec, token_spec)

    return jax.shard_map(local_step, mesh=mesh, in_specs=in_specs, out_specs=token_spec, check_vma=False)
```

```python
import functools

import jax
import jax.numpy as jnp
from jax import lax
from jax.experimental import pallas as pl
from jax.experimental.pallas import tpu as pltpu
from jax.sharding import PartitionSpec as P


BIG, SMALL = 512, 256
CHUNK = 256
TOKENS = 512
VMEM_LIMIT = 58 * 1024 * 1024


def ffn_kernel(carried, split, table, fill, x_ref, gate_ref, up_ref, down_ref, *refs):
    p, f = pl.program_id(0), pl.program_id(1)
    refs = refs[1:] if carried else refs
    outs, total = refs[:-1], refs[-1]
    rows_filled = fill[table[0, p], table[1, p]] * table[3, p]

    def tile(start, size):
        rows = pl.ds(pl.multiple_of(start, SMALL), size)
        x = x_ref[0, 0, rows, :]
        a = jnp.dot(x, gate_ref[0], preferred_element_type=jnp.float32)
        b = jnp.dot(x, up_ref[0], preferred_element_type=jnp.float32)
        h = (jax.nn.silu(a) * b).astype(jnp.bfloat16)
        y = jnp.dot(h, down_ref[0], preferred_element_type=jnp.float32)
        total[rows, :] = jnp.where(f == 0, 0.0, total[rows, :]) + y

    units = (rows_filled + SMALL - 1) >> 8
    pairs = units >> 1

    def pair(i, carry):
        tile(i * BIG, BIG)
        return carry

    lax.fori_loop(0, pairs, pair, 0)

    @pl.when((units & 1) == 1)
    def _():
        tile(pairs * BIG, SMALL)

    def write(y_ref):
        def store(i, carry):
            rows = pl.ds(pl.multiple_of(i * SMALL, SMALL), SMALL)
            slot = i * SMALL + lax.broadcasted_iota(jnp.int32, (SMALL, 1), 0)
            y_ref[0, 0, rows, :] = jnp.where(slot < rows_filled, total[rows, :], 0.0).astype(jnp.bfloat16)
            return carry

        lax.fori_loop(0, units, store, 0)

    last = f == pl.num_programs(1) - 1
    if len(outs) == 1:
        @pl.when(last)
        def _():
            write(outs[0])
    else:
        @pl.when(last & (p < split))
        def _():
            write(outs[0])

        @pl.when(last & (p >= split))
        def _():
            write(outs[1])


def ffn(table, fill, results, x, w_gate, w_up, w_down, carried=None, width=512):
    _, experts, capacity, hidden = x.shape
    width_all = w_gate.shape[2]
    last = width_all // width - 1

    def slice_of(p, f, t):
        return jnp.where(t[3, p] == 1, f, last)

    weight = pl.BlockSpec((1, hidden, width), lambda p, f, t, n: (t[1, p], 0, slice_of(p, f, t)))
    block = (1, 1, capacity, hidden)
    if len(results) == 1:
        out_specs = [pl.BlockSpec(block, lambda p, f, t, n: (t[2, p], t[1, p], 0, 0))]
    else:
        out_specs = [
            pl.BlockSpec(block, lambda p, f, t, n: (0, jnp.minimum(p, 1), 0, 0)),
            pl.BlockSpec(block, lambda p, f, t, n: (t[2, p], t[1, jnp.maximum(p, 2)], 0, 0)),
        ]
    in_specs = [
        pl.BlockSpec(block, lambda p, f, t, n: (t[0, p], t[1, p], 0, 0)),
        weight,
        weight,
        pl.BlockSpec((1, width, hidden), lambda p, f, t, n: (t[1, p], slice_of(p, f, t), 0)),
    ]
    operands = [table, fill, x, w_gate, w_up, w_down]
    if carried is not None:
        in_specs.append(pl.BlockSpec(memory_space=pl.ANY))
        operands.append(carried)
    return pl.pallas_call(
        functools.partial(ffn_kernel, carried is not None, 2),
        out_shape=[jax.ShapeDtypeStruct((n, experts, capacity, hidden), jnp.bfloat16) for n in results],
        grid_spec=pltpu.PrefetchScalarGridSpec(
            num_scalar_prefetch=2,
            grid=(table.shape[1], last + 1),
            in_specs=in_specs,
            out_specs=out_specs,
            scratch_shapes=[pltpu.VMEM((capacity, hidden), jnp.float32)],
        ),
        input_output_aliases={6: 0} if carried is not None else {},
        compiler_params=pltpu.CompilerParams(
            dimension_semantics=("arbitrary", "arbitrary"), vmem_limit_bytes=VMEM_LIMIT
        ),
        cost_estimate=pl.CostEstimate(
            flops=6 * 1536 * hidden * width_all, bytes_accessed=12 * hidden * width_all, transcendentals=0
        ),
    )(*operands)


def combine_kernel(final, out_tiles, info, meta_ref, own_ref, part_ref, *refs):
    if final:
        helped_ref, z0a_ref, z0b_ref, z1a_ref, z1b_ref, out_ref, total = refs
    else:
        out_ref, total = refs
    q, t = pl.program_id(0), pl.program_id(1)
    tokens = pl.ds(pl.multiple_of(t * TOKENS, TOKENS), TOKENS)
    lane = lax.broadcasted_iota(jnp.int32, (TOKENS, meta_ref.shape[1]), 1)
    meta = meta_ref[...]
    column = q ^ info[8]
    slot = jnp.sum(jnp.where(lane == column, meta, 0.0), axis=1, keepdims=True)
    scale = jnp.sum(jnp.where(lane == column + 4, meta, 0.0), axis=1, keepdims=True)

    @pl.when((q == 0) & (info[7] == 1))
    def _():
        total[tokens, :] = jnp.zeros((TOKENS, total.shape[1]), jnp.float32)

    def add_from(ref):
        def add(k, carry):
            rows = pl.ds(pl.multiple_of(k * CHUNK, CHUNK), CHUNK)
            ids = (k * CHUNK + lax.broadcasted_iota(jnp.int32, (TOKENS, CHUNK), 1)).astype(jnp.float32)
            select = jnp.where(slot == ids, 1.0, 0.0).astype(jnp.bfloat16)
            picked = jnp.dot(select, ref[0, 0, rows, :], preferred_element_type=jnp.float32)
            total[tokens, :] += scale * picked
            return carry

        lax.fori_loop(0, (info[q] + CHUNK - 1) >> 8, add, 0)

    @pl.when(q < 2)
    def _():
        add_from(own_ref)

    if final:
        @pl.when((q >= 2) & (info[6] == 0))
        def _():
            add_from(part_ref)

        @pl.when((q >= 2) & (info[6] == 1))
        def _():
            add_from(helped_ref)
    else:
        @pl.when(q >= 2)
        def _():
            add_from(part_ref)

    @pl.when((q == 3) & (info[7] == 1))
    def _():
        if final:
            back = jnp.sum(jnp.where(lane == 8, meta, 0.0), axis=1, keepdims=True)

            def finish(z_ref):
                z = jnp.where(back > 0.0, z_ref[...].astype(jnp.float32), 0.0)
                out_ref[...] = (total[tokens, :] + back * z).astype(jnp.bfloat16)

            half = out_tiles // 2
            for core, low, high in ((0, z0a_ref, z0b_ref), (1, z1a_ref, z1b_ref)):
                pl.when((info[5] == core) & (t < half))(functools.partial(finish, low))
                pl.when((info[5] == core) & (t >= half))(functools.partial(finish, high))
        else:
            out_ref[...] = total[tokens, :].astype(jnp.bfloat16)


def combine(final, info, meta, own, part, *more):
    capacity, hidden = own.shape[2:]
    count, lanes = meta.shape
    block = (1, 1, capacity, hidden)
    half = count // TOKENS // 2
    in_specs = [
        pl.BlockSpec((TOKENS, lanes), lambda q, t, i: (t * i[7], 0)),
        pl.BlockSpec(block, lambda q, t, i: (i[4], jnp.minimum(q, 1) * i[7], 0, 0)),
        pl.BlockSpec(block, lambda q, t, i: (0, jnp.maximum(q - 2, 0) * i[7], 0, 0)),
    ]
    if final:
        in_specs += [
            pl.BlockSpec(block, lambda q, t, i: (0, jnp.maximum(q - 2, 0) * i[6], 0, 0)),
            *(
                pl.BlockSpec(
                    (TOKENS, hidden),
                    lambda q, t, i, core=core, base=base: (
                        jnp.where((q == 3) & (i[5] == core), jnp.clip(t - base, 0, half - 1), 0), 0
                    ),
                    pipeline_mode=pl.Buffered(1),
                )
                for core in (0, 1)
                for base in (0, half)
            ),
        ]
    return pl.pallas_call(
        functools.partial(combine_kernel, final, count // TOKENS),
        out_shape=jax.ShapeDtypeStruct((count, hidden), jnp.bfloat16),
        grid_spec=pltpu.PrefetchScalarGridSpec(
            num_scalar_prefetch=1,
            grid=(4, count // TOKENS),
            in_specs=in_specs,
            out_specs=pl.BlockSpec((TOKENS, hidden), lambda q, t, i: (jnp.where(q == 3, t * i[7], 0), 0)),
            scratch_shapes=[pltpu.VMEM((count, hidden), jnp.float32)],
        ),
        compiler_params=pltpu.CompilerParams(
            dimension_semantics=("arbitrary", "arbitrary"), vmem_limit_bytes=VMEM_LIMIT
        ),
        cost_estimate=pl.CostEstimate(
            flops=2 * 2048 * count * hidden, bytes_accessed=32 * count * hidden, transcendentals=0
        ),
    )(info, meta, own, part, *more)


def routing_meta(experts, slot_index, expert_id, gate_weight, on_chip, raw_single):
    here = (expert_id[:, :, None] == experts) & (slot_index >= 0)[:, :, None]
    slot = jnp.sum(jnp.where(here, slot_index[:, :, None] + 1, 0), axis=1) - 1
    factor = jnp.sum(jnp.where(here, gate_weight[:, :, None], 0.0), axis=1)
    if raw_single:
        factor = jnp.where(on_chip[:, None] == 2, factor, 1.0)
    return jnp.concatenate([slot.astype(jnp.float32), factor], axis=1)


def solution(mesh):
    def local_step(dispatched, w_gate, w_up, w_down, fill_count, slot_index, expert_id, gate_weight):
        me = lax.axis_index("ep")
        core, chip = me & 1, me >> 1
        partner = me ^ 1
        first = 2 * (1 - chip)
        swap_core = [(0, 1), (1, 0), (2, 3), (3, 2)]
        swap_chip = [(0, 2), (2, 0), (1, 3), (3, 1)]

        def permute(value, pairs):
            return lax.ppermute(value, "ep", pairs)

        fill_there = permute(fill_count, swap_core)
        load_here, load_there = jnp.sum(fill_count), jnp.sum(fill_there)
        i_help = load_here + jnp.sum(fill_there[me]) < load_there
        get_help = load_there + jnp.sum(fill_count[partner]) < load_here

        valid = slot_index >= 0
        on_far = jnp.sum((valid & ((expert_id >> 2) != chip)).astype(jnp.int32), axis=1)
        pair_order = jnp.array([0, 1, 2, 3], jnp.int32)

        def chip_experts(owner):
            return jnp.where(pair_order < 2, 2 * owner + pair_order, 2 * (owner ^ 1) + pair_order - 2)

        far_meta = routing_meta(4 * (1 - chip) + pair_order, slot_index, expert_id, gate_weight, on_far, True)
        near_meta = routing_meta(chip_experts(me), slot_index, expert_id, gate_weight, on_far, False)
        far_weight = jnp.sum(jnp.where(valid & ((expert_id >> 2) != chip), gate_weight, 0.0), axis=1)
        back = jnp.where(on_far == 2, 1.0, jnp.where(on_far == 1, far_weight, 0.0))
        near_meta = jnp.concatenate([near_meta, back[:, None]], axis=1)
        halves = far_meta.reshape(2, far_meta.shape[0] // 2, far_meta.shape[1])
        straight = permute(jnp.where(core == 0, halves[0], halves[1]), swap_chip)
        crossed = permute(jnp.where(core == 0, halves[1], halves[0]), [(0, 3), (3, 0), (1, 2), (2, 1)])
        first_meta = jnp.where(core == 0, straight, crossed)
        second_meta = jnp.where(core == 0, crossed, straight)

        def table(sources, places, active):
            passes = 2 * len(sources)
            row = lax.broadcasted_iota(jnp.int32, (4, passes), 0)
            column = lax.broadcasted_iota(jnp.int32, (4, passes), 1)

            def spread(values):
                return values[0] if len(values) == 1 else jnp.where(column < 2, values[0], values[1])

            return jnp.where(
                row == 0,
                spread(sources),
                jnp.where(row == 1, jnp.where(spread(active) == 1, column & 1, 1), jnp.where(row == 2, spread(places), spread(active))),
            ).astype(jnp.int32)

        def info(source, helped):
            fills = jnp.concatenate([fill_count[source], fill_there[source]])
            return jnp.concatenate([fills, jnp.stack([zero, core, helped, one, zero])]).astype(jnp.int32)

        def serve_info(source):
            fills = jnp.concatenate([fill_count[source], fill_there[source]])
            return jnp.concatenate([fills, jnp.stack([zero, core, zero, one, 2 * core])]).astype(jnp.int32)

        zero, one = jnp.int32(0), jnp.int32(1)
        helps = i_help.astype(jnp.int32)
        deferred = get_help.astype(jnp.int32)
        early = 1 - deferred
        gate_there = permute(w_gate, swap_core)
        rows_there = permute(dispatched, swap_core)

        y_first, y_own = ffn(
            table([first, jnp.where(early == 1, me, first)], [zero, zero], [one, early]),
            fill_count,
            (1, 2),
            dispatched,
            w_gate,
            w_up,
            w_down,
        )
        y_first_part = permute(y_first, swap_core)
        up_sent, down_sent, y_first = lax.optimization_barrier((w_up, w_down, y_first))
        up_there = permute(up_sent, swap_core)
        down_there = permute(down_sent, swap_core)
        served0 = combine(False, serve_info(first), first_meta, y_first, y_first_part)
        z0a = permute(served0, [(0, 2), (2, 0)])
        z0b = permute(served0, [(1, 2), (3, 0)])
        second_table = table(
            [first + 1, jnp.where(early == 1, partner, first + 1)], [zero, zero], [one, early]
        )
        second_table, served0 = lax.optimization_barrier((second_table, served0))
        y_second, y_for_partner = ffn(second_table, fill_count, (1, 1), dispatched, w_gate, w_up, w_down)
        y_second_part = permute(y_second, swap_core)
        served1 = combine(False, serve_info(first + 1), second_meta, y_second, y_second_part)
        z1a = permute(served1, [(0, 3), (2, 1)])
        z1b = permute(served1, [(1, 3), (3, 1)])
        y_part = permute(y_for_partner, swap_core)

        local_table = table([me], [early], [deferred])
        local_table, served1 = lax.optimization_barrier((local_table, served1))
        y_own = ffn(local_table, fill_count, (2,), dispatched, w_gate, w_up, w_down, carried=y_own)[0]
        help_table = table([me], [zero], [helps])
        help_table, y_own = lax.optimization_barrier((help_table, y_own))
        y_help = ffn(help_table, fill_there, (1,), rows_there, gate_there, up_there, down_there)[0]
        return combine(True, info(me, helps), near_meta, y_own, y_part, y_help, z0a, z0b, z1a, z1b)

    token_spec = P(("dp", "ep"))
    in_specs = (P("dp", "ep"), P("ep"), P("ep"), P("ep"), P("dp", "ep"), token_spec, token_spec, token_spec)

    return jax.shard_map(local_step, mesh=mesh, in_specs=in_specs, out_specs=token_spec, check_vma=False)
```
